32 devices in a mesh: groups: 2 (over x), seq: 16 (over z, y, core).
Axes of the slice: x: 2, y: 2, z: 4, core: 2. Of those that a mesh axis runs over, the one named last changes fastest.
Arguments:
- first_queries: bfloat16 [4096, 2048], P(('groups', 'seq')), parts along dimension 0, may hold values from -12 to 12
- second_queries: bfloat16 [4096, 2048], P(('groups', 'seq')), parts along dimension 0, may hold values from -12 to 12
- common_keys: bfloat16 [4096, 512], P(('groups', 'seq')), parts along dimension 0, may hold values from -4 to 4
- common_values: bfloat16 [4096, 512], P(('groups', 'seq')), parts along dimension 0, may hold values from -6 to 6
- lengths: int32 [8], P('groups'), parts along dimension 0, may hold values from 1 to 1024, 2048 in all
Outputs:
- first_output: bfloat16 [4096, 2048], P(('groups', 'seq')), parts along dimension 0
- second_output: bfloat16 [4096, 2048], P(('groups', 'seq')), parts along dimension 0
The draws below stay inside these ranges and needn't reach their ends.
There are 2 independent parts, one for each index of `groups`. The reference program is written for one: setup_inputs(seed, part) draws one part's arguments, and reference() takes and returns one part's arrays. A program takes and returns all parts, laid end to end along the dimension named above; each array names one. Nothing has to cross between parts.
Inputs may be any that keep to these rules, and one draw needn't show every extreme that they name: `lengths`: the 4 documents lie end to end in order and fill all 2048 positions.
All inputs are finite; a program needn't handle non-finite values.
Results may differ from the reference program's by a relative error of at most 0.0034.
Values may be sent and summed in bfloat16 or wider, within the bound.
A program may use at most 64 MiB of HBM per device.

```python
import math
import jax
import jax.numpy as jnp
import numpy as np
from jax import lax

HEAD_WIDTH = 128
QUERY_HEAD_COUNT = 16
KEY_VALUE_HEADS = 4
NDOC = 4
GROUP_TOKENS = 2048


def query_draw(key, salt_value):
    random_seed_key = jax.random.fold_in(key, salt_value)
    random_jitter = jnp.clip(2.0 * jax.random.normal(random_seed_key, (GROUP_TOKENS, QUERY_HEAD_COUNT * HEAD_WIDTH), jnp.float32), -8.0, 8.0)
    return random_jitter.astype(jnp.bfloat16)


def draw_first_queries(key, part):
    return query_draw(key, 21)


def draw_second_queries(key, part):
    return query_draw(key, 22)


def draw_common_keys(key, part):
    random_seed_key = jax.random.fold_in(key, 31)
    random_jitter = jnp.clip(jax.random.normal(random_seed_key, (GROUP_TOKENS, KEY_VALUE_HEADS * HEAD_WIDTH), jnp.float32), -4.0, 4.0)
    return random_jitter.astype(jnp.bfloat16)


def block_levels(key, shape, split, least, largest):
    def one(dim, parts):
        steps = jax.random.uniform(jax.random.fold_in(jax.random.fold_in(key, 6), dim), (parts,), jnp.float32, least / len(split), largest / len(split))
        return jnp.repeat(jnp.exp(steps), shape[dim] // parts).reshape((-1,) + (1,) * (len(shape) - dim - 1))

    level = one(*split[0])
    for cut in split[1:]:
        level = level * one(*cut)
    return level


def split_up(amount, total, reach, slope):
    loads = [(1 << 20) // math.isqrt(grade ** slope) + 1 for grade in range(2, amount + 1)]
    rest, given = total - reach - (amount - 1), [1] * (amount - 1)
    while rest > 0:
        movable = [i for i in range(amount - 1) if given[i] < reach]
        whole, budget = sum([loads[i] for i in movable]), rest
        for i in movable:
            addition = min(reach - given[i], max(1, budget * loads[i] // whole), rest)
            given[i] = given[i] + addition
            rest = rest - addition
    return np.array([reach] + given)


def ragged_sizes(stream_key, count, total, most, slope):
    if count == 2:
        one = jax.random.randint(stream_key, (), max(1, total - most), min(most, total - 1) + 1)
        return jnp.stack([one, total - one])
    tallies = jnp.asarray(split_up(count, total, most, slope), jnp.int32)
    twos = (count - 1) // 2
    donor, sink = tallies[1:1 + 2 * twos:2], tallies[2:2 + 2 * twos:2]
    margin = jnp.minimum(donor - 1, most - sink)
    passed = jax.random.randint(jax.random.fold_in(stream_key, 1), (twos,), 0, 1 << 20) % (margin + 1)
    tallies = tallies.at[1:1 + 2 * twos:2].set(donor - passed).at[2:2 + 2 * twos:2].set(sink + passed)
    return tallies[jax.random.permutation(jax.random.fold_in(stream_key, 2), count)]


def scatter_about(own_key, shape, spread, most, cuts=(), kind=jnp.bfloat16):
    drawn = spread * jax.random.normal(own_key, shape, jnp.float32)
    if cuts:
        drawn = drawn * block_levels(own_key, shape, cuts, -0.22, 0.18)
    return jnp.clip(drawn, -most, most).astype(kind)


def setup_inputs(seed: int = 0, part: int = 0) -> dict:
    keys = jax.random.split(jax.random.key(seed), 6)
    part_splits = jax.random.split(jax.random.fold_in(keys[5], part), 6)
    return {
        "first_queries": draw_first_queries(jax.random.fold_in(jax.random.fold_in(keys[5], part), 71), part),
        "second_queries": draw_second_queries(jax.random.fold_in(jax.random.fold_in(keys[5], part), 71), part),
        "common_keys": draw_common_keys(jax.random.fold_in(jax.random.fold_in(keys[5], part), 71), part),
        "common_values": scatter_about(part_splits[3], (GROUP_TOKENS, KEY_VALUE_HEADS * HEAD_WIDTH), 1.0, 6.0, ((0, 16),)),
        "lengths": ragged_sizes(part_splits[4], NDOC, GROUP_TOKENS, GROUP_TOKENS // 2, 2).astype(jnp.int32),
    }


def reference(first_queries, second_queries, common_keys, common_values, lengths):
    positions = jnp.arange(GROUP_TOKENS, dtype=jnp.int32)
    bounds = jnp.cumsum(lengths)
    documents = jnp.sum((positions[:, None] >= bounds[None, :-1]).astype(jnp.int32), axis=1)
    visible = (positions[None, :] <= positions[:, None]) & (documents[None, :] == documents[:, None])
    key_head_count = common_keys.astype(jnp.float32).reshape(GROUP_TOKENS, KEY_VALUE_HEADS, HEAD_WIDTH).transpose(1, 0, 2)
    value_head_count = common_values.astype(jnp.float32).reshape(GROUP_TOKENS, KEY_VALUE_HEADS, HEAD_WIDTH).transpose(1, 0, 2)

    def attend_layer(queries):
        query_heads = queries.astype(jnp.float32).reshape(GROUP_TOKENS, QUERY_HEAD_COUNT, HEAD_WIDTH).transpose(1, 0, 2)

        def one_head(head_position):
            query_head = query_heads[head_position]
            shared_tensor = head_position // (QUERY_HEAD_COUNT // KEY_VALUE_HEADS)
            scores = jnp.einsum("qd,kd->qk", query_head, key_head_count[shared_tensor]) * (HEAD_WIDTH ** -0.5)
            masked = jnp.where(visible, scores, -1e30)
            highest = jnp.max(masked, axis=1, keepdims=True)
            weights = jnp.where(visible, jnp.exp(masked - highest), 0.0)
            row_total = jnp.sum(weights, axis=1, keepdims=True)
            rounded = lax.optimization_barrier(weights.astype(jnp.bfloat16)).astype(jnp.float32)
            blended = jnp.einsum("qk,kd->qd", rounded, value_head_count[shared_tensor])
            return (blended / row_total).astype(jnp.bfloat16)

        head_outputs = lax.map(one_head, jnp.arange(QUERY_HEAD_COUNT, dtype=jnp.int32))
        return head_outputs.transpose(1, 0, 2).reshape(GROUP_TOKENS, QUERY_HEAD_COUNT * HEAD_WIDTH)

    return attend_layer(first_queries), attend_layer(second_queries)
```

```python
import functools
import math

import jax
import jax.numpy as jnp
from jax import lax
from jax.experimental import pallas as pl
from jax.experimental.pallas import tpu as pltpu
from jax.sharding import PartitionSpec as P

HEAD_WIDTH = 128
QUERY_HEAD_COUNT = 16
KEY_VALUE_HEADS = 4
SHARE = QUERY_HEAD_COUNT // KEY_VALUE_HEADS
PLANE = 4
CHUNKS = 2
TILE = 256
CORES = 2
REACH = 4
Y_LAG = 3
Z_PAIR_LAG = 2
Y_PAIR_LAG = 5
SUM_ROWS = 16
HIDDEN = -1e30
MESH = pl.DeviceIdType.MESH


def wide_kernel(
    members,
    hops,
    lengths_ref,
    first_ref,
    second_ref,
    keys_ref,
    values_ref,
    first_out,
    second_out,
    key_buffer,
    value_buffer,
    turned,
    bias,
    highest,
    total,
    send_sem,
    recv_sem,
):
    group = lax.axis_index("groups")
    me = lax.axis_index("seq")
    planes = members // PLANE
    plane = me // PLANE
    column = me % PLANE
    base = plane * PLANE
    beside = column + 1 - 2 * (column % 2)
    across = (column + 2) % PLANE
    corner = (beside + 2) % PLANE
    rows = keys_ref.shape[0]
    chunk_width = keys_ref.shape[1] // CHUNKS
    own = (keys_ref, values_ref)
    buffers = (key_buffer, value_buffer)
    has_upper = plane + 1 < planes
    has_lower = plane >= 1

    barrier = pltpu.get_barrier_semaphore()

    def greet(seat):
        pl.semaphore_signal(barrier, inc=1, device_id=(group, seat), device_id_type=MESH)

    greet(base + beside)
    greet(base + across)

    @pl.when(has_upper)
    def _():
        greet(me + PLANE)

    @pl.when(has_lower)
    def _():
        greet(me - PLANE)

    pl.semaphore_wait(barrier, 2 + has_upper.astype(jnp.int32) + has_lower.astype(jnp.int32))

    def wanted(hop, source, target):
        if hop == 0:
            return source < target
        if hop == hops:
            return (source > target) & (plane >= hop)
        return plane >= hop

    def slot(kind, hop, seat, chunk):
        start = pl.multiple_of(((hops - hop) * PLANE + seat) * rows, rows)
        return buffers[kind].at[pl.ds(start, rows), pl.ds(chunk * chunk_width, chunk_width)]

    def held(kind, hop, seat, chunk):
        if hop == 0:
            return own[kind].at[:, pl.ds(chunk * chunk_width, chunk_width)]
        return slot(kind, hop, seat, chunk)

    pending = []

    def send(condition, source, destination, target, index):
        @pl.when(condition)
        def _():
            pltpu.make_async_remote_copy(
                src_ref=source,
                dst_ref=destination,
                send_sem=send_sem.at[index],
                recv_sem=recv_sem.at[index],
                device_id=(group, target),
                device_id_type=MESH,
            ).start()

        pending.append((condition, source, destination, target, index))

    def receive(condition, destination, index):
        @pl.when(condition)
        def _():
            pltpu.make_async_remote_copy(
                src_ref=destination,
                dst_ref=destination,
                send_sem=send_sem.at[index],
                recv_sem=recv_sem.at[index],
                device_id=(group, base + beside),
                device_id_type=MESH,
            ).wait_recv()

    def send_up(hop, chunk, kind):
        send(
            has_upper & (plane >= hop - 1),
            held(kind, hop - 1, column, chunk),
            slot(kind, hop, column, chunk),
            me + PLANE,
            (kind, hop, 0, chunk),
        )

    def send_across(hop, chunk, kind):
        send(
            wanted(hop, column, across),
            held(kind, hop, column, chunk),
            slot(kind, hop, column, chunk),
            base + across,
            (kind, hop, 2, chunk),
        )

    def send_beside(hop, chunk, kind):
        send(
            wanted(hop, column, beside),
            held(kind, hop, column, chunk),
            slot(kind, hop, column, chunk),
            base + beside,
            (kind, hop, 1, chunk),
        )

    def pass_beside(hop, chunk, kind):
        send(
            wanted(hop, across, beside),
            slot(kind, hop, across, chunk),
            slot(kind, hop, across, chunk),
            base + beside,
            (kind, hop, 3, chunk),
        )

    def take_up(hop, chunk, kind):
        receive(plane >= hop, slot(kind, hop, column, chunk), (kind, hop, 0, chunk))

    def take_across(hop, chunk, kind):
        receive(
            wanted(hop, across, column),
            slot(kind, hop, across, chunk),
            (kind, hop, 2, chunk),
        )

    def take_beside(hop, chunk, kind):
        receive(
            wanted(hop, beside, column),
            slot(kind, hop, beside, chunk),
            (kind, hop, 1, chunk),
        )
        receive(
            wanted(hop, corner, column),
            slot(kind, hop, corner, chunk),
            (kind, hop, 3, chunk),
        )

    for chunk in range(CHUNKS):
        for kind in range(2):
            send_up(1, chunk, kind)
            send_across(0, chunk, kind)
            send_beside(0, chunk, kind)

    own_start = pl.multiple_of((hops * PLANE + column) * rows, rows)
    key_buffer[pl.ds(own_start, rows), :] = keys_ref[...]
    value_buffer[pl.ds(own_start, rows), :] = values_ref[...]
    nothing = jnp.zeros(keys_ref.shape, keys_ref.dtype)
    for seat in range(PLANE):

        @pl.when(seat > column)
        def _():
            start = (hops * PLANE + seat) * rows
            key_buffer[pl.ds(start, rows), :] = nothing
            value_buffer[pl.ds(start, rows), :] = nothing

        @pl.when((seat < column) & (plane >= hops))
        def _():
            start = seat * rows
            key_buffer[pl.ds(start, rows), :] = nothing
            value_buffer[pl.ds(start, rows), :] = nothing

    place = lax.broadcasted_iota(jnp.int32, (1, rows), 1) + me * rows
    bound = jnp.int32(0)
    begin = jnp.zeros((1, rows), jnp.int32)
    for document in range(lengths_ref.shape[0] - 1):
        bound = bound + lengths_ref[document]
        begin = jnp.where(place >= bound, bound, begin)
    plane_rows = PLANE * rows
    for hop in range(hops + 1):
        key_place = lax.broadcasted_iota(jnp.int32, (plane_rows, rows), 0) + (
            (plane - hop) * plane_rows
        )
        visible = (key_place >= begin) & (key_place <= place)
        bias[pl.ds((hops - hop) * plane_rows, plane_rows), :] = jnp.where(
            visible, 0.0, HIDDEN
        )

    queries = (first_ref, second_ref)
    outputs = (first_out, second_out)
    stacked = 2 * SHARE * rows

    def turn(head, carry):
        for layer in range(2):
            for member in range(SHARE):
                start = pl.multiple_of((head * SHARE + member) * HEAD_WIDTH, HEAD_WIDTH)
                piece = queries[layer][:, pl.ds(start, HEAD_WIDTH)]
                turned[head, :, pl.ds((layer * SHARE + member) * rows, rows)] = piece.T
        return carry

    lax.fori_loop(0, KEY_VALUE_HEADS, turn, 0)

    factor = HEAD_WIDTH ** (-0.5) * math.log2(math.e)
    heads_per_chunk = KEY_VALUE_HEADS // CHUNKS

    def absorb(first_row, key_rows, fresh, head):
        columns = pl.ds(pl.multiple_of(head * HEAD_WIDTH, HEAD_WIDTH), HEAD_WIDTH)
        tile_keys = key_buffer[pl.ds(first_row, key_rows), columns]
        tile_values = value_buffer[pl.ds(first_row, key_rows), columns]
        flat_values = jnp.concatenate(
            [tile_values.T, jnp.ones((SUM_ROWS, key_rows), tile_values.dtype)], axis=0
        )
        hidden = bias[pl.ds(first_row, key_rows), :]
        hidden = jnp.concatenate([hidden] * (TILE // rows), axis=1)

        def score(start):
            span = pl.ds(start, TILE)
            scores = jnp.dot(tile_keys, turned[head, :, span], preferred_element_type=jnp.float32)
            masked = scores + hidden
            top = jnp.max(masked, axis=0, keepdims=True)
            if not fresh:
                top = jnp.maximum(top, highest[head, :, span])
            return masked, top

        def blend(start, weights, top):
            span = pl.ds(start, TILE)
            product = jnp.dot(flat_values, weights, preferred_element_type=jnp.float32)
            if not fresh:
                before = highest[head, :, span]
                product = product + total[head, :, span] * jnp.exp2((before - top) * factor)
            highest[head, :, span] = top
            total[head, :, span] = product

        starts = list(range(0, stacked, TILE))
        upcoming = score(starts[0])
        earlier = None
        for place_in, start in enumerate(starts):
            masked, top = upcoming
            if place_in + 1 < len(starts):
                upcoming = score(starts[place_in + 1])
            weights = jnp.exp2((masked - top) * factor).astype(jnp.bfloat16)
            if earlier is not None:
                blend(*earlier)
            earlier = (start, weights, top)
        blend(*earlier)

    def attend(hop, chunk):
        first_row = (hops - hop) * plane_rows
        half = plane_rows // 2

        def over(first, count):
            def step(index, carry):
                absorb(first, count, hop == 0, chunk * heads_per_chunk + index)
                return carry

            lax.fori_loop(0, heads_per_chunk, step, 0)

        if hop == 0:

            @pl.when(column < PLANE // 2)
            def _():
                over(first_row, half)

            @pl.when(column >= PLANE // 2)
            def _():
                over(first_row, plane_rows)
        elif hop == hops:

            @pl.when((plane >= hop) & (column < PLANE // 2))
            def _():
                over(first_row, plane_rows)

            @pl.when((plane >= hop) & (column >= PLANE // 2))
            def _():
                over(first_row + half, half)
        else:

            @pl.when(plane >= hop)
            def _():
                over(first_row, plane_rows)

    def finish(chunk):
        def step(index, carry):
            head = chunk * heads_per_chunk + index
            for layer in range(2):
                for member in range(SHARE):
                    span = pl.ds((layer * SHARE + member) * rows, rows)
                    weighted = total[head, 0:HEAD_WIDTH, span]
                    mass = total[head, HEAD_WIDTH : HEAD_WIDTH + 1, span]
                    blended = (weighted / mass).astype(jnp.bfloat16)
                    start = pl.multiple_of((head * SHARE + member) * HEAD_WIDTH, HEAD_WIDTH)
                    outputs[layer][:, pl.ds(start, HEAD_WIDTH)] = blended.T
            return carry

        lax.fori_loop(0, heads_per_chunk, step, 0)

    for hop in range(hops + 1):
        for chunk in range(CHUNKS):
            for kind in range(2):
                if hop < hops:
                    take_up(hop + 1, chunk, kind)
                    if hop + 2 <= hops:
                        send_up(hop + 2, chunk, kind)
                    send_across(hop + 1, chunk, kind)
                    send_beside(hop + 1, chunk, kind)
                take_across(hop, chunk, kind)
                pass_beside(hop, chunk, kind)
            for kind in range(2):
                take_beside(hop, chunk, kind)
            attend(hop, chunk)
            if hop == hops:
                finish(chunk)

    for condition, source, destination, target, index in pending:

        @pl.when(condition)
        def _():
            pltpu.make_async_remote_copy(
                src_ref=source,
                dst_ref=destination,
                send_sem=send_sem.at[index],
                recv_sem=recv_sem.at[index],
                device_id=(group, target),
                device_id_type=MESH,
            ).wait_send()


def on_device_wide(first_queries, second_queries, common_keys, common_values, lengths):
    members = lax.axis_size("seq")
    hops = members // (2 * PLANE)
    rows = common_keys.shape[0]
    slots = (hops + 1) * PLANE
    width = common_keys.shape[1]
    stacked = 2 * SHARE * rows
    in_vmem = pl.BlockSpec(memory_space=pltpu.VMEM)
    shape = jax.ShapeDtypeStruct(first_queries.shape, jnp.bfloat16)
    semaphores = pltpu.SemaphoreType.DMA((2, hops + 1, 4, CHUNKS))
    return pl.pallas_call(
        functools.partial(wide_kernel, members, hops),
        out_shape=(shape, shape),
        in_specs=[pl.BlockSpec(memory_space=pltpu.SMEM)] + [in_vmem] * 4,
        out_specs=(in_vmem, in_vmem),
        scratch_shapes=[
            pltpu.VMEM((slots * rows, width), jnp.bfloat16),
            pltpu.VMEM((slots * rows, width), jnp.bfloat16),
            pltpu.VMEM((KEY_VALUE_HEADS, HEAD_WIDTH, stacked), jnp.bfloat16),
            pltpu.VMEM((slots * rows, rows), jnp.float32),
            pltpu.VMEM((KEY_VALUE_HEADS, 1, stacked), jnp.float32),
            pltpu.VMEM((KEY_VALUE_HEADS, HEAD_WIDTH + SUM_ROWS, stacked), jnp.float32),
            semaphores,
            semaphores,
        ],
        compiler_params=pltpu.CompilerParams(collective_id=0, has_side_effects=True),
    )(lengths, first_queries, second_queries, common_keys, common_values)


def kernel(
    planes,
    lengths_ref,
    first_ref,
    second_ref,
    keys_ref,
    values_ref,
    first_out,
    second_out,
    queries,
    held,
    bias,
    scores,
    weights,
    tops,
    highest,
    total,
    own_sem,
    query_sem,
    z_send,
    z_recv,
    y_send,
    y_recv,
    pair_send,
    pair_recv,
):
    group = lax.axis_index("groups")
    me = lax.axis_index("seq")
    plane = me // PLANE
    column = (me // CORES) % 2
    core = me % CORES
    chip = me // CORES
    partner = me + 1 - 2 * core
    beside = me + CORES - 2 * CORES * column
    rows = keys_ref.shape[0]
    unit = CORES * rows
    stacked = 2 * SHARE * rows
    factor = HEAD_WIDTH ** (-0.5) * math.log2(math.e)
    has_upper = plane + 1 < planes
    items = 4 * KEY_VALUE_HEADS

    def slot(kind, head, distance):
        start = pl.multiple_of(distance * unit + core * rows, rows)
        return held.at[kind, head, pl.ds(start, rows), :]

    def parts_of(item):
        return item // (2 * KEY_VALUE_HEADS), (item // KEY_VALUE_HEADS) % 2, item % KEY_VALUE_HEADS

    def own_copy(kind, head):
        return pltpu.make_async_copy(
            (keys_ref, values_ref)[kind].at[:, pl.ds(head * HEAD_WIDTH, HEAD_WIDTH)],
            slot(kind, head, 0),
            own_sem.at[kind, head],
        )

    def query_copy(layer, head):
        start = pl.multiple_of(head * HEAD_WIDTH, HEAD_WIDTH)
        first = pl.multiple_of((layer * SHARE + head % SHARE) * rows, rows)
        return pltpu.make_async_copy(
            (first_ref, second_ref)[layer].at[:, pl.ds(start, HEAD_WIDTH)],
            queries.at[head // SHARE, pl.ds(first, rows), :],
            query_sem.at[layer, head],
        )

    barrier = pltpu.get_barrier_semaphore()

    def greet(seat):
        pl.semaphore_signal(barrier, inc=1, device_id=(group, seat), device_id_type=MESH)

    @pl.when(plane >= 1)
    def _():
        greet(me - PLANE)

    @pl.when(plane >= 1 - column)
    def _():
        greet(beside)

    greet(partner)

    for head in range(KEY_VALUE_HEADS):
        own_copy(0, head).start()
    for head in range(KEY_VALUE_HEADS):
        own_copy(1, head).start()

    def load_queries(head, carry):
        for layer in range(2):
            query_copy(layer, head).start()
        return carry

    lax.fori_loop(0, QUERY_HEAD_COUNT, load_queries, 0)

    def remote(source, target_slot, send_sem, recv_sem, seat):
        return pltpu.make_async_remote_copy(
            src_ref=source,
            dst_ref=target_slot,
            send_sem=send_sem,
            recv_sem=recv_sem,
            device_id=(group, seat),
            device_id_type=MESH,
        )

    def z_copy(item):
        kind, hop, head = parts_of(item)
        return remote(
            slot(kind, head, 2 * hop),
            slot(kind, head, 2 * hop + 2),
            z_send.at[item],
            z_recv.at[item],
            me + PLANE,
        )

    def y_copy(item):
        kind, half, head = parts_of(item)
        return remote(
            slot(kind, head, 2 * half + 2 * column),
            slot(kind, head, 2 * half + 1),
            y_send.at[item],
            y_recv.at[item],
            beside,
        )

    def pair_copy(kind, distance, head):
        place = slot(kind, head, distance)
        index = (kind, distance, head)
        return remote(place, place, pair_send.at[index], pair_recv.at[index], partner)

    def y_sends(half):
        return plane >= half + column

    def y_takes(half):
        return plane >= half + 1 - column

    def start_own(kind):
        @pl.when(has_upper)
        def _():
            for head in range(KEY_VALUE_HEADS):
                z_copy(kind * 2 * KEY_VALUE_HEADS + head).start()

        @pl.when(column == 0)
        def _():
            for head in range(KEY_VALUE_HEADS):
                y_copy(kind * 2 * KEY_VALUE_HEADS + head).start()

    pl.semaphore_wait(
        barrier, 1 + has_upper.astype(jnp.int32) + (plane >= column).astype(jnp.int32)
    )
    for head in range(KEY_VALUE_HEADS):
        own_copy(0, head).wait()
    start_own(0)
    for head in range(KEY_VALUE_HEADS):
        pair_copy(0, 0, head).start()
    for head in range(KEY_VALUE_HEADS):
        own_copy(1, head).wait()
    for head in range(KEY_VALUE_HEADS):
        pair_copy(1, 0, head).start()

    @pl.when(plane == 0)
    def _():
        start_own(1)

    place = lax.broadcasted_iota(jnp.int32, (rows, unit), 0) + me * rows
    bound = jnp.int32(0)
    begin = jnp.zeros((rows, unit), jnp.int32)
    for document in range(lengths_ref.shape[0] - 1):
        bound = bound + lengths_ref[document]
        begin = jnp.where(place >= bound, bound, begin)
    for distance in range(REACH + 1):
        key_place = lax.broadcasted_iota(jnp.int32, (rows, unit), 1) + (chip - distance) * unit
        visible = (key_place >= begin) & (key_place <= place)
        bias[distance] = jnp.where(visible, 0.0, HIDDEN)

    def unit_rows(distance):
        return pl.ds(pl.multiple_of(distance * unit, unit), unit)

    def weigh(head, distance, fresh, room):
        keys = held[0, head, unit_rows(distance), :]
        half = stacked // 2
        for first in range(0, stacked, half):
            scores[room, pl.ds(first, half), :] = lax.dot_general(
                queries[head, pl.ds(first, half), :],
                keys,
                (((1,), (1,)), ((), ())),
                preferred_element_type=jnp.float32,
            )
        step = rows // 2
        for first in range(0, stacked, step):
            span = pl.ds(first, step)
            masked = scores[room, span, :] + bias[distance, pl.ds(first % rows, step), :]
            top = jnp.max(masked, axis=1, keepdims=True)
            weights[head, distance, span, :] = jnp.exp2((masked - top) * factor).astype(
                jnp.bfloat16
            )
            spread = jnp.broadcast_to(top, (step, HEAD_WIDTH))
            tops[head, distance, span, :] = spread
            if fresh:
                highest[head, span, :] = spread
            else:
                highest[head, span, :] = jnp.maximum(highest[head, span, :], spread)

    def blend(head, distance, fresh):
        values = held[1, head, unit_rows(distance), :]
        product = jnp.dot(
            weights[head, distance],
            jnp.concatenate([values, jnp.ones_like(values)], axis=1),
            preferred_element_type=jnp.float32,
        )
        step = rows // 2
        for first in range(0, stacked, step):
            span = pl.ds(first, step)
            share = jnp.exp2((tops[head, distance, span, :] - highest[head, span, :]) * factor)
            part = product[first : first + step] * jnp.concatenate([share, share], axis=1)
            if fresh:
                total[head, span, :] = part
            else:
                total[head, span, :] = total[head, span, :] + part

    outputs = (first_out, second_out)

    def finish(head):
        for layer in range(2):
            for member in range(SHARE):
                span = pl.ds((layer * SHARE + member) * rows, rows)
                blended = total[head, span, 0:HEAD_WIDTH] / total[head, span, HEAD_WIDTH:]
                start = pl.multiple_of((head * SHARE + member) * HEAD_WIDTH, HEAD_WIDTH)
                outputs[layer][:, pl.ds(start, HEAD_WIDTH)] = blended.astype(jnp.bfloat16)

    def wait_queries(head, carry):
        for layer in range(2):
            query_copy(layer, head).wait()
        return carry

    lax.fori_loop(0, QUERY_HEAD_COUNT, wait_queries, 0)

    def nearest(head, carry):
        pair_copy(0, 0, head).wait_recv()
        weigh(head, 0, True, 0)
        return carry

    lax.fori_loop(0, KEY_VALUE_HEADS, nearest, 0)

    y_last = items - 1 + Y_PAIR_LAG
    settle = 2 * KEY_VALUE_HEADS - KEY_VALUE_HEADS + Y_PAIR_LAG

    def step(index, carry):
        kind, hop, head = parts_of(index)

        @pl.when((index < items) & (plane >= hop + 1))
        def _():
            z_copy(index).wait_recv()

            @pl.when(column == 1)
            def _():
                y_copy(index).start()

            @pl.when((column == 0) & (hop == 0))
            def _():
                y_copy(index + KEY_VALUE_HEADS).start()

            @pl.when(has_upper & (hop == 0))
            def _():
                z_copy(index + KEY_VALUE_HEADS).start()

            pair_copy(kind, 2 * hop + 2, head).start()

        @pl.when((index == KEY_VALUE_HEADS - 1) & (plane >= 1))
        def _():
            start_own(1)

        y_item = index - Y_LAG
        y_kind, y_half, y_head = parts_of(y_item)

        @pl.when((y_item >= 0) & (y_item < items) & y_takes(y_half))
        def _():
            y_copy(y_item).wait_recv()
            pair_copy(y_kind, 2 * y_half + 1, y_head).start()

        pair_item = index - Z_PAIR_LAG
        pair_kind, pair_hop, pair_head = parts_of(pair_item)

        @pl.when((pair_item >= 0) & (pair_item < items) & (plane >= pair_hop + 1))
        def _():
            distance = 2 * pair_hop + 2
            pair_copy(pair_kind, distance, pair_head).wait_recv()

            @pl.when(pair_kind == 0)
            def _():
                weigh(pair_head, distance, False, 0)

            @pl.when(pair_kind == 1)
            def _():
                blend(pair_head, distance, False)

        late_item = index - Y_PAIR_LAG
        late_kind, late_half, late_head = parts_of(late_item)

        @pl.when((late_item >= 0) & y_takes(late_half))
        def _():
            distance = 2 * late_half + 1
            pair_copy(late_kind, distance, late_head).wait_recv()

            @pl.when(late_kind == 0)
            def _():
                weigh(late_head, distance, False, 1)

            @pl.when(late_kind == 1)
            def _():
                blend(late_head, distance, False)

        @pl.when((index >= settle) & (index < settle + KEY_VALUE_HEADS))
        def _():
            pair_copy(1, 0, index - settle).wait_recv()
            blend(index - settle, 0, True)

        @pl.when(index >= y_last + 1 - KEY_VALUE_HEADS)
        def _():
            finish(index - (y_last + 1 - KEY_VALUE_HEADS))

        return carry

    lax.fori_loop(0, y_last + 1, step, 0)

    def settle_sends(item, carry):
        kind, hop, head = parts_of(item)

        @pl.when(has_upper & (plane >= hop))
        def _():
            z_copy(item).wait_send()

        @pl.when(y_sends(hop))
        def _():
            y_copy(item).wait_send()

        return carry

    lax.fori_loop(0, items, settle_sends, 0)
    for distance in range(REACH + 1):

        @pl.when(chip >= distance)
        def _():
            for kind in range(2):
                for head in range(KEY_VALUE_HEADS):
                    pair_copy(kind, distance, head).wait_send()


def on_device(first_queries, second_queries, common_keys, common_values, lengths):
    planes = lax.axis_size("seq") // PLANE
    rows = common_keys.shape[0]
    unit = CORES * rows
    units = REACH + 1
    stacked = 2 * SHARE * rows
    in_vmem = pl.BlockSpec(memory_space=pltpu.VMEM)
    anywhere = pl.BlockSpec(memory_space=pl.ANY)
    shape = jax.ShapeDtypeStruct(first_queries.shape, jnp.bfloat16)
    link_sems = pltpu.SemaphoreType.DMA((4 * KEY_VALUE_HEADS,))
    pair_sems = pltpu.SemaphoreType.DMA((2, units, KEY_VALUE_HEADS))
    return pl.pallas_call(
        functools.partial(kernel, planes),
        out_shape=(shape, shape),
        in_specs=[pl.BlockSpec(memory_space=pltpu.SMEM)] + [anywhere] * 4,
        out_specs=(in_vmem, in_vmem),
        scratch_shapes=[
            pltpu.VMEM((KEY_VALUE_HEADS, stacked, HEAD_WIDTH), jnp.bfloat16),
            pltpu.VMEM((2, KEY_VALUE_HEADS, units * unit, HEAD_WIDTH), jnp.bfloat16),
            pltpu.VMEM((units, rows, unit), jnp.float32),
            pltpu.VMEM((2, stacked, unit), jnp.float32),
            pltpu.VMEM((KEY_VALUE_HEADS, units, stacked, unit), jnp.bfloat16),
            pltpu.VMEM((KEY_VALUE_HEADS, units, stacked, HEAD_WIDTH), jnp.float32),
            pltpu.VMEM((KEY_VALUE_HEADS, stacked, HEAD_WIDTH), jnp.float32),
            pltpu.VMEM((KEY_VALUE_HEADS, stacked, 2 * HEAD_WIDTH), jnp.float32),
            pltpu.SemaphoreType.DMA((2, KEY_VALUE_HEADS)),
            pltpu.SemaphoreType.DMA((2, QUERY_HEAD_COUNT)),
            link_sems,
            link_sems,
            link_sems,
            link_sems,
            pair_sems,
            pair_sems,
        ],
        compiler_params=pltpu.CompilerParams(collective_id=0, has_side_effects=True),
    )(lengths, first_queries, second_queries, common_keys, common_values)


def solution(mesh):
    in_specs = (
        P(("groups", "seq"), None),
        P(("groups", "seq"), None),
        P(("groups", "seq"), None),
        P(("groups", "seq"), None),
        P("groups"),
    )
    out_specs = (P(("groups", "seq"), None), P(("groups", "seq"), None))
    body = on_device if mesh.shape["seq"] == 2 * REACH * CORES else on_device_wide
    return jax.shard_map(
        body, mesh=mesh, in_specs=in_specs, out_specs=out_specs, check_vma=False
    )
```

```python
import functools
import math

import jax
import jax.numpy as jnp
from jax import lax
from jax.experimental import pallas as pl
from jax.experimental.pallas import tpu as pltpu
from jax.sharding import PartitionSpec as P

HEAD_WIDTH = 128
QUERY_HEAD_COUNT = 16
KEY_VALUE_HEADS = 4
SHARE = QUERY_HEAD_COUNT // KEY_VALUE_HEADS
PLANE = 4
CHUNKS = 2
TILE = 256
CORES = 2
REACH = 4
DISTANCES = (0, 2, 1, 4, 3)
TEAMS = ((0, 2), (2, 2), (4, 1))
Y_LAG = 5
Z_PAIR_LAG = 2
Y_PAIR_LAG = 7
WEIGH_STEPS = (2, 7, 11)
BLEND_STEPS = (12, 15, 19)
SUM_ROWS = 16
HIDDEN = -1e30
MESH = pl.DeviceIdType.MESH


def wide_kernel(
    members,
    hops,
    lengths_ref,
    first_ref,
    second_ref,
    keys_ref,
    values_ref,
    first_out,
    second_out,
    key_buffer,
    value_buffer,
    turned,
    bias,
    highest,
    total,
    send_sem,
    recv_sem,
):
    group = lax.axis_index("groups")
    me = lax.axis_index("seq")
    planes = members // PLANE
    plane = me // PLANE
    column = me % PLANE
    base = plane * PLANE
    beside = column + 1 - 2 * (column % 2)
    across = (column + 2) % PLANE
    corner = (beside + 2) % PLANE
    rows = keys_ref.shape[0]
    chunk_width = keys_ref.shape[1] // CHUNKS
    own = (keys_ref, values_ref)
    buffers = (key_buffer, value_buffer)
    has_upper = plane + 1 < planes
    has_lower = plane >= 1

    barrier = pltpu.get_barrier_semaphore()

    def greet(seat):
        pl.semaphore_signal(barrier, inc=1, device_id=(group, seat), device_id_type=MESH)

    greet(base + beside)
    greet(base + across)

    @pl.when(has_upper)
    def _():
        greet(me + PLANE)

    @pl.when(has_lower)
    def _():
        greet(me - PLANE)

    pl.semaphore_wait(barrier, 2 + has_upper.astype(jnp.int32) + has_lower.astype(jnp.int32))

    def wanted(hop, source, target):
        if hop == 0:
            return source < target
        if hop == hops:
            return (source > target) & (plane >= hop)
        return plane >= hop

    def slot(kind, hop, seat, chunk):
        start = pl.multiple_of(((hops - hop) * PLANE + seat) * rows, rows)
        return buffers[kind].at[pl.ds(start, rows), pl.ds(chunk * chunk_width, chunk_width)]

    def held(kind, hop, seat, chunk):
        if hop == 0:
            return own[kind].at[:, pl.ds(chunk * chunk_width, chunk_width)]
        return slot(kind, hop, seat, chunk)

    pending = []

    def send(condition, source, destination, target, index):
        @pl.when(condition)
        def _():
            pltpu.make_async_remote_copy(
                src_ref=source,
                dst_ref=destination,
                send_sem=send_sem.at[index],
                recv_sem=recv_sem.at[index],
                device_id=(group, target),
                device_id_type=MESH,
            ).start()

        pending.append((condition, source, destination, target, index))

    def receive(condition, destination, index):
        @pl.when(condition)
        def _():
            pltpu.make_async_remote_copy(
                src_ref=destination,
                dst_ref=destination,
                send_sem=send_sem.at[index],
                recv_sem=recv_sem.at[index],
                device_id=(group, base + beside),
                device_id_type=MESH,
            ).wait_recv()

    def send_up(hop, chunk, kind):
        send(
            has_upper & (plane >= hop - 1),
            held(kind, hop - 1, column, chunk),
            slot(kind, hop, column, chunk),
            me + PLANE,
            (kind, hop, 0, chunk),
        )

    def send_across(hop, chunk, kind):
        send(
            wanted(hop, column, across),
            held(kind, hop, column, chunk),
            slot(kind, hop, column, chunk),
            base + across,
            (kind, hop, 2, chunk),
        )

    def send_beside(hop, chunk, kind):
        send(
            wanted(hop, column, beside),
            held(kind, hop, column, chunk),
            slot(kind, hop, column, chunk),
            base + beside,
            (kind, hop, 1, chunk),
        )

    def pass_beside(hop, chunk, kind):
        send(
            wanted(hop, across, beside),
            slot(kind, hop, across, chunk),
            slot(kind, hop, across, chunk),
            base + beside,
            (kind, hop, 3, chunk),
        )

    def take_up(hop, chunk, kind):
        receive(plane >= hop, slot(kind, hop, column, chunk), (kind, hop, 0, chunk))

    def take_across(hop, chunk, kind):
        receive(
            wanted(hop, across, column),
            slot(kind, hop, across, chunk),
            (kind, hop, 2, chunk),
        )

    def take_beside(hop, chunk, kind):
        receive(
            wanted(hop, beside, column),
            slot(kind, hop, beside, chunk),
            (kind, hop, 1, chunk),
        )
        receive(
            wanted(hop, corner, column),
            slot(kind, hop, corner, chunk),
            (kind, hop, 3, chunk),
        )

    for chunk in range(CHUNKS):
        for kind in range(2):
            send_up(1, chunk, kind)
            send_across(0, chunk, kind)
            send_beside(0, chunk, kind)

    own_start = pl.multiple_of((hops * PLANE + column) * rows, rows)
    key_buffer[pl.ds(own_start, rows), :] = keys_ref[...]
    value_buffer[pl.ds(own_start, rows), :] = values_ref[...]
    nothing = jnp.zeros(keys_ref.shape, keys_ref.dtype)
    for seat in range(PLANE):

        @pl.when(seat > column)
        def _():
            start = (hops * PLANE + seat) * rows
            key_buffer[pl.ds(start, rows), :] = nothing
            value_buffer[pl.ds(start, rows), :] = nothing

        @pl.when((seat < column) & (plane >= hops))
        def _():
            start = seat * rows
            key_buffer[pl.ds(start, rows), :] = nothing
            value_buffer[pl.ds(start, rows), :] = nothing

    place = lax.broadcasted_iota(jnp.int32, (1, rows), 1) + me * rows
    bound = jnp.int32(0)
    begin = jnp.zeros((1, rows), jnp.int32)
    for document in range(lengths_ref.shape[0] - 1):
        bound = bound + lengths_ref[document]
        begin = jnp.where(place >= bound, bound, begin)
    plane_rows = PLANE * rows
    for hop in range(hops + 1):
        key_place = lax.broadcasted_iota(jnp.int32, (plane_rows, rows), 0) + (
            (plane - hop) * plane_rows
        )
        visible = (key_place >= begin) & (key_place <= place)
        bias[pl.ds((hops - hop) * plane_rows, plane_rows), :] = jnp.where(
            visible, 0.0, HIDDEN
        )

    queries = (first_ref, second_ref)
    outputs = (first_out, second_out)
    stacked = 2 * SHARE * rows

    def turn(head, carry):
        for layer in range(2):
            for member in range(SHARE):
                start = pl.multiple_of((head * SHARE + member) * HEAD_WIDTH, HEAD_WIDTH)
                piece = queries[layer][:, pl.ds(start, HEAD_WIDTH)]
                turned[head, :, pl.ds((layer * SHARE + member) * rows, rows)] = piece.T
        return carry

    lax.fori_loop(0, KEY_VALUE_HEADS, turn, 0)

    factor = HEAD_WIDTH ** (-0.5) * math.log2(math.e)
    heads_per_chunk = KEY_VALUE_HEADS // CHUNKS

    def absorb(first_row, key_rows, fresh, head):
        columns = pl.ds(pl.multiple_of(head * HEAD_WIDTH, HEAD_WIDTH), HEAD_WIDTH)
        tile_keys = key_buffer[pl.ds(first_row, key_rows), columns]
        tile_values = value_buffer[pl.ds(first_row, key_rows), columns]
        flat_values = jnp.concatenate(
            [tile_values.T, jnp.ones((SUM_ROWS, key_rows), tile_values.dtype)], axis=0
        )
        hidden = bias[pl.ds(first_row, key_rows), :]
        hidden = jnp.concatenate([hidden] * (TILE // rows), axis=1)

        def score(start):
            span = pl.ds(start, TILE)
            scores = jnp.dot(tile_keys, turned[head, :, span], preferred_element_type=jnp.float32)
            masked = scores + hidden
            top = jnp.max(masked, axis=0, keepdims=True)
            if not fresh:
                top = jnp.maximum(top, highest[head, :, span])
            return masked, top

        def blend(start, weights, top):
            span = pl.ds(start, TILE)
            product = jnp.dot(flat_values, weights, preferred_element_type=jnp.float32)
            if not fresh:
                before = highest[head, :, span]
                product = product + total[head, :, span] * jnp.exp2((before - top) * factor)
            highest[head, :, span] = top
            total[head, :, span] = product

        starts = list(range(0, stacked, TILE))
        upcoming = score(starts[0])
        earlier = None
        for place_in, start in enumerate(starts):
            masked, top = upcoming
            if place_in + 1 < len(starts):
                upcoming = score(starts[place_in + 1])
            weights = jnp.exp2((masked - top) * factor).astype(jnp.bfloat16)
            if earlier is not None:
                blend(*earlier)
            earlier = (start, weights, top)
        blend(*earlier)

    def attend(hop, chunk):
        first_row = (hops - hop) * plane_rows
        half = plane_rows // 2

        def over(first, count):
            def step(index, carry):
                absorb(first, count, hop == 0, chunk * heads_per_chunk + index)
                return carry

            lax.fori_loop(0, heads_per_chunk, step, 0)

        if hop == 0:

            @pl.when(column < PLANE // 2)
            def _():
                over(first_row, half)

            @pl.when(column >= PLANE // 2)
            def _():
                over(first_row, plane_rows)
        elif hop == hops:

            @pl.when((plane >= hop) & (column < PLANE // 2))
            def _():
                over(first_row, plane_rows)

            @pl.when((plane >= hop) & (column >= PLANE // 2))
            def _():
                over(first_row + half, half)
        else:

            @pl.when(plane >= hop)
            def _():
                over(first_row, plane_rows)

    def finish(chunk):
        def step(index, carry):
            head = chunk * heads_per_chunk + index
            for layer in range(2):
                for member in range(SHARE):
                    span = pl.ds((layer * SHARE + member) * rows, rows)
                    weighted = total[head, 0:HEAD_WIDTH, span]
                    mass = total[head, HEAD_WIDTH : HEAD_WIDTH + 1, span]
                    blended = (weighted / mass).astype(jnp.bfloat16)
                    start = pl.multiple_of((head * SHARE + member) * HEAD_WIDTH, HEAD_WIDTH)
                    outputs[layer][:, pl.ds(start, HEAD_WIDTH)] = blended.T
            return carry

        lax.fori_loop(0, heads_per_chunk, step, 0)

    for hop in range(hops + 1):
        for chunk in range(CHUNKS):
            for kind in range(2):
                if hop < hops:
                    take_up(hop + 1, chunk, kind)
                    if hop + 2 <= hops:
                        send_up(hop + 2, chunk, kind)
                    send_across(hop + 1, chunk, kind)
                    send_beside(hop + 1, chunk, kind)
                take_across(hop, chunk, kind)
                pass_beside(hop, chunk, kind)
            for kind in range(2):
                take_beside(hop, chunk, kind)
            attend(hop, chunk)
            if hop == hops:
                finish(chunk)

    for condition, source, destination, target, index in pending:

        @pl.when(condition)
        def _():
            pltpu.make_async_remote_copy(
                src_ref=source,
                dst_ref=destination,
                send_sem=send_sem.at[index],
                recv_sem=recv_sem.at[index],
                device_id=(group, target),
                device_id_type=MESH,
            ).wait_send()


def on_device_wide(first_queries, second_queries, common_keys, common_values, lengths):
    members = lax.axis_size("seq")
    hops = members // (2 * PLANE)
    rows = common_keys.shape[0]
    slots = (hops + 1) * PLANE
    width = common_keys.shape[1]
    stacked = 2 * SHARE * rows
    in_vmem = pl.BlockSpec(memory_space=pltpu.VMEM)
    shape = jax.ShapeDtypeStruct(first_queries.shape, jnp.bfloat16)
    semaphores = pltpu.SemaphoreType.DMA((2, hops + 1, 4, CHUNKS))
    return pl.pallas_call(
        functools.partial(wide_kernel, members, hops),
        out_shape=(shape, shape),
        in_specs=[pl.BlockSpec(memory_space=pltpu.SMEM)] + [in_vmem] * 4,
        out_specs=(in_vmem, in_vmem),
        scratch_shapes=[
            pltpu.VMEM((slots * rows, width), jnp.bfloat16),
            pltpu.VMEM((slots * rows, width), jnp.bfloat16),
            pltpu.VMEM((KEY_VALUE_HEADS, HEAD_WIDTH, stacked), jnp.bfloat16),
            pltpu.VMEM((slots * rows, rows), jnp.float32),
            pltpu.VMEM((KEY_VALUE_HEADS, 1, stacked), jnp.float32),
            pltpu.VMEM((KEY_VALUE_HEADS, HEAD_WIDTH + SUM_ROWS, stacked), jnp.float32),
            semaphores,
            semaphores,
        ],
        compiler_params=pltpu.CompilerParams(collective_id=0, has_side_effects=True),
    )(lengths, first_queries, second_queries, common_keys, common_values)


def kernel(
    planes,
    lengths_ref,
    first_ref,
    second_ref,
    keys_ref,
    values_ref,
    first_out,
    second_out,
    queries,
    held,
    bias,
    scores,
    weights,
    tops,
    highest,
    total,
    own_sem,
    query_sem,
    z_send,
    z_recv,
    y_send,
    y_recv,
    pair_send,
    pair_recv,
):
    group = lax.axis_index("groups")
    me = lax.axis_index("seq")
    plane = me // PLANE
    column = (me // CORES) % 2
    core = me % CORES
    chip = me // CORES
    partner = me + 1 - 2 * core
    beside = me + CORES - 2 * CORES * column
    rows = keys_ref.shape[0]
    unit = CORES * rows
    stacked = 2 * SHARE * rows
    factor = HEAD_WIDTH ** (-0.5) * math.log2(math.e)
    has_upper = plane + 1 < planes
    items = 4 * KEY_VALUE_HEADS

    def slot(kind, head, position):
        start = pl.multiple_of(position * unit + core * rows, rows)
        return held.at[kind, head, pl.ds(start, rows), :]

    def parts_of(item):
        return item // (2 * KEY_VALUE_HEADS), (item // KEY_VALUE_HEADS) % 2, item % KEY_VALUE_HEADS

    def own_copy(kind, head):
        return pltpu.make_async_copy(
            (keys_ref, values_ref)[kind].at[:, pl.ds(head * HEAD_WIDTH, HEAD_WIDTH)],
            slot(kind, head, 0),
            own_sem.at[kind],
        )

    def query_copy(layer, head):
        start = pl.multiple_of(head * HEAD_WIDTH, HEAD_WIDTH)
        first = pl.multiple_of((layer * SHARE + head % SHARE) * rows, rows)
        return pltpu.make_async_copy(
            (first_ref, second_ref)[layer].at[:, pl.ds(start, HEAD_WIDTH)],
            queries.at[head // SHARE, pl.ds(first, rows), :],
            query_sem,
        )

    barrier = pltpu.get_barrier_semaphore()

    def greet(seat):
        pl.semaphore_signal(barrier, inc=1, device_id=(group, seat), device_id_type=MESH)

    @pl.when(plane >= 1)
    def _():
        greet(me - PLANE)

    @pl.when(plane >= 1 - column)
    def _():
        greet(beside)

    greet(partner)

    for head in range(KEY_VALUE_HEADS):
        own_copy(0, head).start()
    for head in range(KEY_VALUE_HEADS):
        own_copy(1, head).start()

    def load_queries(head, carry):
        for layer in range(2):
            query_copy(layer, head).start()
        return carry

    lax.fori_loop(0, QUERY_HEAD_COUNT, load_queries, 0)

    def remote(source, target_slot, send_sem, recv_sem, seat):
        return pltpu.make_async_remote_copy(
            src_ref=source,
            dst_ref=target_slot,
            send_sem=send_sem,
            recv_sem=recv_sem,
            device_id=(group, seat),
            device_id_type=MESH,
        )

    def z_copy(item):
        kind, hop, head = parts_of(item)
        return remote(
            slot(kind, head, hop),
            slot(kind, head, 2 * hop + 1),
            z_send.at[hop],
            z_recv.at[item],
            me + PLANE,
        )

    def y_copy(item):
        kind, half, head = parts_of(item)
        return remote(
            slot(kind, head, half + column * (half + 1)),
            slot(kind, head, 2 * half + 2),
            y_send.at[half],
            y_recv.at[item],
            beside,
        )

    def pair_copy(kind, position, head):
        place = slot(kind, head, position)
        index = (kind, position, head)
        return remote(place, place, pair_send.at[position], pair_recv.at[index], partner)

    def all_sent(sem):
        every = held.at[:, :, pl.ds(0, rows), :]
        remote(every, every, sem, sem, partner).wait_send()

    def own_arrived(kind):
        every = held.at[kind, :, pl.ds(pl.multiple_of(core * rows, rows), rows), :]
        pltpu.make_async_copy(every, every, own_sem.at[kind]).wait()

    def y_sends(half):
        return plane >= half + column

    def y_takes(half):
        return plane >= half + 1 - column

    def start_own(kind):
        @pl.when(has_upper)
        def _():
            for head in range(KEY_VALUE_HEADS):
                z_copy(kind * 2 * KEY_VALUE_HEADS + head).start()

        @pl.when(column == 0)
        def _():
            for head in range(KEY_VALUE_HEADS):
                y_copy(kind * 2 * KEY_VALUE_HEADS + head).start()

    pl.semaphore_wait(
        barrier, 1 + has_upper.astype(jnp.int32) + (plane >= column).astype(jnp.int32)
    )
    own_arrived(0)
    start_own(0)
    for head in range(KEY_VALUE_HEADS):
        pair_copy(0, 0, head).start()
    own_arrived(1)
    for head in range(KEY_VALUE_HEADS):
        pair_copy(1, 0, head).start()

    @pl.when(plane == 0)
    def _():
        start_own(1)

    place = lax.broadcasted_iota(jnp.int32, (rows, unit), 0) + me * rows
    bound = jnp.int32(0)
    begin = jnp.zeros((rows, unit), jnp.int32)
    for document in range(lengths_ref.shape[0] - 1):
        bound = bound + lengths_ref[document]
        begin = jnp.where(place >= bound, bound, begin)
    nothing = jnp.zeros((2, KEY_VALUE_HEADS, unit, HEAD_WIDTH), held.dtype)
    for position, distance in enumerate(DISTANCES):
        spot = pl.ds(position * unit, unit)
        key_place = lax.broadcasted_iota(jnp.int32, (rows, unit), 1) + (chip - distance) * unit
        visible = (key_place >= begin) & (key_place <= place)
        bias[:, spot] = jnp.where(visible, 0.0, HIDDEN)

        @pl.when(chip < distance)
        def _():
            held[:, :, spot, :] = nothing

    def weigh(head, team):
        spot = pl.ds(TEAMS[team][0] * unit, TEAMS[team][1] * unit)
        width = TEAMS[team][1] * unit
        keys = held[0, head, spot, :]
        half = stacked // 2
        for first in range(0, stacked, half):
            scores[pl.ds(first, half), 0:width] = lax.dot_general(
                queries[head, pl.ds(first, half), :],
                keys,
                (((1,), (1,)), ((), ())),
                preferred_element_type=jnp.float32,
            )
        step = rows // 4
        for first in range(0, stacked, step):
            span = pl.ds(first, step)
            masked = scores[span, 0:width] + bias[pl.ds(first % rows, step), spot]
            top = jnp.max(masked, axis=1, keepdims=True)
            weights[head, span, spot] = jnp.exp2((masked - top) * factor).astype(jnp.bfloat16)
            spread = jnp.broadcast_to(top, (step, HEAD_WIDTH))
            tops[head, team, span, :] = spread
            if team == 0:
                highest[head, span, :] = spread
            else:
                highest[head, span, :] = jnp.maximum(highest[head, span, :], spread)

    def blend(head, team):
        spot = pl.ds(TEAMS[team][0] * unit, TEAMS[team][1] * unit)
        values = held[1, head, spot, :]
        product = jnp.dot(
            weights[head, :, spot],
            jnp.concatenate([values, jnp.ones_like(values)], axis=1),
            preferred_element_type=jnp.float32,
        )
        step = rows // 2
        for first in range(0, stacked, step):
            span = pl.ds(first, step)
            share = jnp.exp2((tops[head, team, span, :] - highest[head, span, :]) * factor)
            part = product[first : first + step] * jnp.concatenate([share, share], axis=1)
            if team == 0:
                total[head, span, :] = part
            else:
                total[head, span, :] = total[head, span, :] + part

    outputs = (first_out, second_out)

    def finish(head):
        for layer in range(2):
            for member in range(SHARE):
                span = pl.ds((layer * SHARE + member) * rows, rows)
                blended = total[head, span, 0:HEAD_WIDTH] / total[head, span, HEAD_WIDTH:]
                start = pl.multiple_of((head * SHARE + member) * HEAD_WIDTH, HEAD_WIDTH)
                outputs[layer][:, pl.ds(start, HEAD_WIDTH)] = blended.astype(jnp.bfloat16)

    pltpu.make_async_copy(queries, queries, query_sem).wait()

    def at(index, begin, stages):
        return (index >= begin) & (index < begin + stages)

    def z_ready(item):
        kind, hop, head = parts_of(item)

        @pl.when((item >= 0) & (item < items) & (plane >= hop + 1))
        def _():
            pair_copy(kind, 2 * hop + 1, head).wait_recv()

    def y_ready(item):
        kind, half, head = parts_of(item)

        @pl.when((item >= 0) & (item < items) & y_takes(half))
        def _():
            pair_copy(kind, 2 * half + 2, head).wait_recv()

    def step(index, carry):
        kind, hop, head = parts_of(index)

        @pl.when((index < items) & (plane >= hop + 1))
        def _():
            z_copy(index).wait_recv()

            @pl.when(column == 1)
            def _():
                y_copy(index).start()

            @pl.when((column == 0) & (hop == 0))
            def _():
                y_copy(index + KEY_VALUE_HEADS).start()

            @pl.when(has_upper & (hop == 0))
            def _():
                z_copy(index + KEY_VALUE_HEADS).start()

            pair_copy(kind, 2 * hop + 1, head).start()

        @pl.when((index == KEY_VALUE_HEADS - 1) & (plane >= 1))
        def _():
            start_own(1)

        y_item = index - Y_LAG
        y_kind, y_half, y_head = parts_of(y_item)

        @pl.when((y_item >= 0) & (y_item < items) & y_takes(y_half))
        def _():
            y_copy(y_item).wait_recv()
            pair_copy(y_kind, 2 * y_half + 2, y_head).start()

        z_ready(index - Z_PAIR_LAG)
        y_ready(index - Y_PAIR_LAG)

        for kind_done, stages in ((0, WEIGH_STEPS), (1, BLEND_STEPS)):
            for team, begin in enumerate(stages):

                @pl.when(at(index, begin, KEY_VALUE_HEADS))
                def _():
                    if team == 0:
                        pair_copy(kind_done, 0, index - begin).wait_recv()
                    (weigh, blend)[kind_done](index - begin, team)

        @pl.when(at(index, BLEND_STEPS[-1], KEY_VALUE_HEADS))
        def _():
            finish(index - BLEND_STEPS[-1])

        return carry

    lax.fori_loop(0, BLEND_STEPS[-1] + KEY_VALUE_HEADS, step, 0)

    for hop in range(2):

        @pl.when(has_upper & (plane >= hop))
        def _():
            all_sent(z_send.at[hop])

        @pl.when(y_sends(hop))
        def _():
            all_sent(y_send.at[hop])

    for position, distance in enumerate(DISTANCES):

        @pl.when(chip >= distance)
        def _():
            all_sent(pair_send.at[position])


def on_device(first_queries, second_queries, common_keys, common_values, lengths):
    planes = lax.axis_size("seq") // PLANE
    rows = common_keys.shape[0]
    unit = CORES * rows
    units = REACH + 1
    stacked = 2 * SHARE * rows
    in_vmem = pl.BlockSpec(memory_space=pltpu.VMEM)
    anywhere = pl.BlockSpec(memory_space=pl.ANY)
    shape = pltpu.VMEM(first_queries.shape, jnp.bfloat16)
    placed = pl.pallas_call(
        functools.partial(kernel, planes),
        out_shape=(shape, shape),
        in_specs=[pl.BlockSpec(memory_space=pltpu.SMEM)] + [anywhere] * 4,
        out_specs=(in_vmem, in_vmem),
        scratch_shapes=[
            pltpu.VMEM((KEY_VALUE_HEADS, stacked, HEAD_WIDTH), jnp.bfloat16),
            pltpu.VMEM((2, KEY_VALUE_HEADS, units * unit, HEAD_WIDTH), jnp.bfloat16),
            pltpu.VMEM((rows, units * unit), jnp.float32),
            pltpu.VMEM((stacked, 2 * unit), jnp.float32),
            pltpu.VMEM((KEY_VALUE_HEADS, stacked, units * unit), jnp.bfloat16),
            pltpu.VMEM((KEY_VALUE_HEADS, len(TEAMS), stacked, HEAD_WIDTH), jnp.float32),
            pltpu.VMEM((KEY_VALUE_HEADS, stacked, HEAD_WIDTH), jnp.float32),
            pltpu.VMEM((KEY_VALUE_HEADS, stacked, 2 * HEAD_WIDTH), jnp.float32),
            pltpu.SemaphoreType.DMA((2,)),
            pltpu.SemaphoreType.DMA,
            pltpu.SemaphoreType.DMA((2,)),
            pltpu.SemaphoreType.DMA((4 * KEY_VALUE_HEADS,)),
            pltpu.SemaphoreType.DMA((2,)),
            pltpu.SemaphoreType.DMA((4 * KEY_VALUE_HEADS,)),
            pltpu.SemaphoreType.DMA((units,)),
            pltpu.SemaphoreType.DMA((2, units, KEY_VALUE_HEADS)),
        ],
        compiler_params=pltpu.CompilerParams(collective_id=0, has_side_effects=True),
    )(lengths, first_queries, second_queries, common_keys, common_values)
    return to_memory(*placed)


def place_outputs(first_ref, second_ref, first_out, second_out, sems):
    copies = [
        pltpu.make_async_copy(source, target, sems.at[index])
        for index, (source, target) in enumerate(
            ((first_ref, first_out), (second_ref, second_out))
        )
    ]
    for copy in copies:
        copy.start()
    for copy in copies:
        copy.wait()


def to_memory(first, second):
    in_vmem = pl.BlockSpec(memory_space=pltpu.VMEM)
    anywhere = pl.BlockSpec(memory_space=pltpu.HBM)
    shape = jax.ShapeDtypeStruct(first.shape, first.dtype)
    return pl.pallas_call(
        place_outputs,
        out_shape=(shape, shape),
        in_specs=[in_vmem] * 2,
        out_specs=(anywhere, anywhere),
        scratch_shapes=[pltpu.SemaphoreType.DMA((2,))],
    )(
        pltpu.with_memory_space_constraint(first, pltpu.VMEM),
        pltpu.with_memory_space_constraint(second, pltpu.VMEM),
    )


def solution(mesh):
    in_specs = (
        P(("groups", "seq"), None),
        P(("groups", "seq"), None),
        P(("groups", "seq"), None),
        P(("groups", "seq"), None),
        P("groups"),
    )
    out_specs = (P(("groups", "seq"), None), P(("groups", "seq"), None))
    body = on_device if mesh.shape["seq"] == 2 * REACH * CORES else on_device_wide
    return jax.shard_map(
        body, mesh=mesh, in_specs=in_specs, out_specs=out_specs, check_vma=False
    )
```

```python
import functools
import math

import jax
import jax.numpy as jnp
from jax import lax
from jax.experimental import pallas as pl
from jax.experimental.pallas import tpu as pltpu
from jax.sharding import PartitionSpec as P

HEAD_WIDTH = 128
QUERY_HEAD_COUNT = 16
KEY_VALUE_HEADS = 4
SHARE = QUERY_HEAD_COUNT // KEY_VALUE_HEADS
PLANE = 4
CHUNKS = 2
TILE = 256
CORES = 2
REACH = 4
DISTANCES = (0, 2, 1, 4, 3)
TEAMS = ((0, 2), (2, 2), (4, 1))
BATCH = 2
Y_LAG = 2
Z_PAIR_LAG = 1
Y_PAIR_LAG = 3
WEIGH_STEPS = (1, 3, 5)
BLEND_STEPS = (5, 7, 9)
SUM_ROWS = 16
HIDDEN = -1e30
MESH = pl.DeviceIdType.MESH


def wide_kernel(
    members,
    hops,
    lengths_ref,
    first_ref,
    second_ref,
    keys_ref,
    values_ref,
    first_out,
    second_out,
    key_buffer,
    value_buffer,
    turned,
    bias,
    highest,
    total,
    send_sem,
    recv_sem,
):
    group = lax.axis_index("groups")
    me = lax.axis_index("seq")
    planes = members // PLANE
    plane = me // PLANE
    column = me % PLANE
    base = plane * PLANE
    beside = column + 1 - 2 * (column % 2)
    across = (column + 2) % PLANE
    corner = (beside + 2) % PLANE
    rows = keys_ref.shape[0]
    chunk_width = keys_ref.shape[1] // CHUNKS
    own = (keys_ref, values_ref)
    buffers = (key_buffer, value_buffer)
    has_upper = plane + 1 < planes
    has_lower = plane >= 1

    barrier = pltpu.get_barrier_semaphore()

    def greet(seat):
        pl.semaphore_signal(barrier, inc=1, device_id=(group, seat), device_id_type=MESH)

    greet(base + beside)
    greet(base + across)

    @pl.when(has_upper)
    def _():
        greet(me + PLANE)

    @pl.when(has_lower)
    def _():
        greet(me - PLANE)

    pl.semaphore_wait(barrier, 2 + has_upper.astype(jnp.int32) + has_lower.astype(jnp.int32))

    def wanted(hop, source, target):
        if hop == 0:
            return source < target
        if hop == hops:
            return (source > target) & (plane >= hop)
        return plane >= hop

    def slot(kind, hop, seat, chunk):
        start = pl.multiple_of(((hops - hop) * PLANE + seat) * rows, rows)
        return buffers[kind].at[pl.ds(start, rows), pl.ds(chunk * chunk_width, chunk_width)]

    def held(kind, hop, seat, chunk):
        if hop == 0:
            return own[kind].at[:, pl.ds(chunk * chunk_width, chunk_width)]
        return slot(kind, hop, seat, chunk)

    pending = []

    def send(condition, source, destination, target, index):
        @pl.when(condition)
        def _():
            pltpu.make_async_remote_copy(
                src_ref=source,
                dst_ref=destination,
                send_sem=send_sem.at[index],
                recv_sem=recv_sem.at[index],
                device_id=(group, target),
                device_id_type=MESH,
            ).start()

        pending.append((condition, source, destination, target, index))

    def receive(condition, destination, index):
        @pl.when(condition)
        def _():
            pltpu.make_async_remote_copy(
                src_ref=destination,
                dst_ref=destination,
                send_sem=send_sem.at[index],
                recv_sem=recv_sem.at[index],
                device_id=(group, base + beside),
                device_id_type=MESH,
            ).wait_recv()

    def send_up(hop, chunk, kind):
        send(
            has_upper & (plane >= hop - 1),
            held(kind, hop - 1, column, chunk),
            slot(kind, hop, column, chunk),
            me + PLANE,
            (kind, hop, 0, chunk),
        )

    def send_across(hop, chunk, kind):
        send(
            wanted(hop, column, across),
            held(kind, hop, column, chunk),
            slot(kind, hop, column, chunk),
            base + across,
            (kind, hop, 2, chunk),
        )

    def send_beside(hop, chunk, kind):
        send(
            wanted(hop, column, beside),
            held(kind, hop, column, chunk),
            slot(kind, hop, column, chunk),
            base + beside,
            (kind, hop, 1, chunk),
        )

    def pass_beside(hop, chunk, kind):
        send(
            wanted(hop, across, beside),
            slot(kind, hop, across, chunk),
            slot(kind, hop, across, chunk),
            base + beside,
            (kind, hop, 3, chunk),
        )

    def take_up(hop, chunk, kind):
        receive(plane >= hop, slot(kind, hop, column, chunk), (kind, hop, 0, chunk))

    def take_across(hop, chunk, kind):
        receive(
            wanted(hop, across, column),
            slot(kind, hop, across, chunk),
            (kind, hop, 2, chunk),
        )

    def take_beside(hop, chunk, kind):
        receive(
            wanted(hop, beside, column),
            slot(kind, hop, beside, chunk),
            (kind, hop, 1, chunk),
        )
        receive(
            wanted(hop, corner, column),
            slot(kind, hop, corner, chunk),
            (kind, hop, 3, chunk),
        )

    for chunk in range(CHUNKS):
        for kind in range(2):
            send_up(1, chunk, kind)
            send_across(0, chunk, kind)
            send_beside(0, chunk, kind)

    own_start = pl.multiple_of((hops * PLANE + column) * rows, rows)
    key_buffer[pl.ds(own_start, rows), :] = keys_ref[...]
    value_buffer[pl.ds(own_start, rows), :] = values_ref[...]
    nothing = jnp.zeros(keys_ref.shape, keys_ref.dtype)
    for seat in range(PLANE):

        @pl.when(seat > column)
        def _():
            start = (hops * PLANE + seat) * rows
            key_buffer[pl.ds(start, rows), :] = nothing
            value_buffer[pl.ds(start, rows), :] = nothing

        @pl.when((seat < column) & (plane >= hops))
        def _():
            start = seat * rows
            key_buffer[pl.ds(start, rows), :] = nothing
            value_buffer[pl.ds(start, rows), :] = nothing

    place = lax.broadcasted_iota(jnp.int32, (1, rows), 1) + me * rows
    bound = jnp.int32(0)
    begin = jnp.zeros((1, rows), jnp.int32)
    for document in range(lengths_ref.shape[0] - 1):
        bound = bound + lengths_ref[document]
        begin = jnp.where(place >= bound, bound, begin)
    plane_rows = PLANE * rows
    for hop in range(hops + 1):
        key_place = lax.broadcasted_iota(jnp.int32, (plane_rows, rows), 0) + (
            (plane - hop) * plane_rows
        )
        visible = (key_place >= begin) & (key_place <= place)
        bias[pl.ds((hops - hop) * plane_rows, plane_rows), :] = jnp.where(
            visible, 0.0, HIDDEN
        )

    queries = (first_ref, second_ref)
    outputs = (first_out, second_out)
    stacked = 2 * SHARE * rows

    def turn(head, carry):
        for layer in range(2):
            for member in range(SHARE):
                start = pl.multiple_of((head * SHARE + member) * HEAD_WIDTH, HEAD_WIDTH)
                piece = queries[layer][:, pl.ds(start, HEAD_WIDTH)]
                turned[head, :, pl.ds((layer * SHARE + member) * rows, rows)] = piece.T
        return carry

    lax.fori_loop(0, KEY_VALUE_HEADS, turn, 0)

    factor = HEAD_WIDTH ** (-0.5) * math.log2(math.e)
    heads_per_chunk = KEY_VALUE_HEADS // CHUNKS

    def absorb(first_row, key_rows, fresh, head):
        columns = pl.ds(pl.multiple_of(head * HEAD_WIDTH, HEAD_WIDTH), HEAD_WIDTH)
        tile_keys = key_buffer[pl.ds(first_row, key_rows), columns]
        tile_values = value_buffer[pl.ds(first_row, key_rows), columns]
        flat_values = jnp.concatenate(
            [tile_values.T, jnp.ones((SUM_ROWS, key_rows), tile_values.dtype)], axis=0
        )
        hidden = bias[pl.ds(first_row, key_rows), :]
        hidden = jnp.concatenate([hidden] * (TILE // rows), axis=1)

        def score(start):
            span = pl.ds(start, TILE)
            scores = jnp.dot(tile_keys, turned[head, :, span], preferred_element_type=jnp.float32)
            masked = scores + hidden
            top = jnp.max(masked, axis=0, keepdims=True)
            if not fresh:
                top = jnp.maximum(top, highest[head, :, span])
            return masked, top

        def blend(start, weights, top):
            span = pl.ds(start, TILE)
            product = jnp.dot(flat_values, weights, preferred_element_type=jnp.float32)
            if not fresh:
                before = highest[head, :, span]
                product = product + total[head, :, span] * jnp.exp2((before - top) * factor)
            highest[head, :, span] = top
            total[head, :, span] = product

        starts = list(range(0, stacked, TILE))
        upcoming = score(starts[0])
        earlier = None
        for place_in, start in enumerate(starts):
            masked, top = upcoming
            if place_in + 1 < len(starts):
                upcoming = score(starts[place_in + 1])
            weights = jnp.exp2((masked - top) * factor).astype(jnp.bfloat16)
            if earlier is not None:
                blend(*earlier)
            earlier = (start, weights, top)
        blend(*earlier)

    def attend(hop, chunk):
        first_row = (hops - hop) * plane_rows
        half = plane_rows // 2

        def over(first, count):
            def step(index, carry):
                absorb(first, count, hop == 0, chunk * heads_per_chunk + index)
                return carry

            lax.fori_loop(0, heads_per_chunk, step, 0)

        if hop == 0:

            @pl.when(column < PLANE // 2)
            def _():
                over(first_row, half)

            @pl.when(column >= PLANE // 2)
            def _():
                over(first_row, plane_rows)
        elif hop == hops:

            @pl.when((plane >= hop) & (column < PLANE // 2))
            def _():
                over(first_row, plane_rows)

            @pl.when((plane >= hop) & (column >= PLANE // 2))
            def _():
                over(first_row + half, half)
        else:

            @pl.when(plane >= hop)
            def _():
                over(first_row, plane_rows)

    def finish(chunk):
        def step(index, carry):
            head = chunk * heads_per_chunk + index
            for layer in range(2):
                for member in range(SHARE):
                    span = pl.ds((layer * SHARE + member) * rows, rows)
                    weighted = total[head, 0:HEAD_WIDTH, span]
                    mass = total[head, HEAD_WIDTH : HEAD_WIDTH + 1, span]
                    blended = (weighted / mass).astype(jnp.bfloat16)
                    start = pl.multiple_of((head * SHARE + member) * HEAD_WIDTH, HEAD_WIDTH)
                    outputs[layer][:, pl.ds(start, HEAD_WIDTH)] = blended.T
            return carry

        lax.fori_loop(0, heads_per_chunk, step, 0)

    for hop in range(hops + 1):
        for chunk in range(CHUNKS):
            for kind in range(2):
                if hop < hops:
                    take_up(hop + 1, chunk, kind)
                    if hop + 2 <= hops:
                        send_up(hop + 2, chunk, kind)
                    send_across(hop + 1, chunk, kind)
                    send_beside(hop + 1, chunk, kind)
                take_across(hop, chunk, kind)
                pass_beside(hop, chunk, kind)
            for kind in range(2):
                take_beside(hop, chunk, kind)
            attend(hop, chunk)
            if hop == hops:
                finish(chunk)

    for condition, source, destination, target, index in pending:

        @pl.when(condition)
        def _():
            pltpu.make_async_remote_copy(
                src_ref=source,
                dst_ref=destination,
                send_sem=send_sem.at[index],
                recv_sem=recv_sem.at[index],
                device_id=(group, target),
                device_id_type=MESH,
            ).wait_send()


def on_device_wide(first_queries, second_queries, common_keys, common_values, lengths):
    members = lax.axis_size("seq")
    hops = members // (2 * PLANE)
    rows = common_keys.shape[0]
    slots = (hops + 1) * PLANE
    width = common_keys.shape[1]
    stacked = 2 * SHARE * rows
    in_vmem = pl.BlockSpec(memory_space=pltpu.VMEM)
    shape = jax.ShapeDtypeStruct(first_queries.shape, jnp.bfloat16)
    semaphores = pltpu.SemaphoreType.DMA((2, hops + 1, 4, CHUNKS))
    return pl.pallas_call(
        functools.partial(wide_kernel, members, hops),
        out_shape=(shape, shape),
        in_specs=[pl.BlockSpec(memory_space=pltpu.SMEM)] + [in_vmem] * 4,
        out_specs=(in_vmem, in_vmem),
        scratch_shapes=[
            pltpu.VMEM((slots * rows, width), jnp.bfloat16),
            pltpu.VMEM((slots * rows, width), jnp.bfloat16),
            pltpu.VMEM((KEY_VALUE_HEADS, HEAD_WIDTH, stacked), jnp.bfloat16),
            pltpu.VMEM((slots * rows, rows), jnp.float32),
            pltpu.VMEM((KEY_VALUE_HEADS, 1, stacked), jnp.float32),
            pltpu.VMEM((KEY_VALUE_HEADS, HEAD_WIDTH + SUM_ROWS, stacked), jnp.float32),
            semaphores,
            semaphores,
        ],
        compiler_params=pltpu.CompilerParams(collective_id=0, has_side_effects=True),
    )(lengths, first_queries, second_queries, common_keys, common_values)


def kernel(
    planes,
    lengths_hbm,
    first_ref,
    second_ref,
    keys_ref,
    values_ref,
    first_out,
    second_out,
    queries,
    held,
    bias,
    scores,
    weights,
    tops,
    highest,
    total,
    lengths_ref,
    length_sem,
    own_sem,
    query_sem,
    z_send,
    z_recv,
    y_send,
    y_recv,
    pair_send,
    pair_recv,
):
    group = lax.axis_index("groups")
    me = lax.axis_index("seq")
    plane = me // PLANE
    column = (me // CORES) % 2
    core = me % CORES
    chip = me // CORES
    partner = me + 1 - 2 * core
    beside = me + CORES - 2 * CORES * column
    rows = keys_ref.shape[0]
    unit = CORES * rows
    stacked = 2 * SHARE * rows
    factor = HEAD_WIDTH ** (-0.5) * math.log2(math.e)
    has_upper = plane + 1 < planes
    items = 4 * KEY_VALUE_HEADS

    def slot(kind, head, position):
        start = pl.multiple_of(position * unit + core * rows, rows)
        return held.at[kind, head, pl.ds(start, rows), :]

    def parts_of(item):
        return item // (2 * KEY_VALUE_HEADS), (item // KEY_VALUE_HEADS) % 2, item % KEY_VALUE_HEADS

    def own_copy(kind, head):
        return pltpu.make_async_copy(
            (keys_ref, values_ref)[kind].at[:, pl.ds(head * HEAD_WIDTH, HEAD_WIDTH)],
            slot(kind, head, 0),
            own_sem.at[kind],
        )

    def query_copy(layer, head):
        start = pl.multiple_of(head * HEAD_WIDTH, HEAD_WIDTH)
        first = pl.multiple_of((layer * SHARE + head % SHARE) * rows, rows)
        return pltpu.make_async_copy(
            (first_ref, second_ref)[layer].at[:, pl.ds(start, HEAD_WIDTH)],
            queries.at[head // SHARE, pl.ds(first, rows), :],
            query_sem,
        )

    barrier = pltpu.get_barrier_semaphore()

    def greet(seat):
        pl.semaphore_signal(barrier, inc=1, device_id=(group, seat), device_id_type=MESH)

    @pl.when(plane >= 1)
    def _():
        greet(me - PLANE)

    @pl.when(plane >= 1 - column)
    def _():
        greet(beside)

    greet(partner)

    for head in range(KEY_VALUE_HEADS):
        own_copy(0, head).start()
    length_copy = pltpu.make_async_copy(lengths_hbm, lengths_ref, length_sem)
    length_copy.start()
    for head in range(KEY_VALUE_HEADS):
        own_copy(1, head).start()

    def load_queries(head, carry):
        for layer in range(2):
            query_copy(layer, head).start()
        return carry

    lax.fori_loop(0, QUERY_HEAD_COUNT, load_queries, 0)

    def remote(source, target_slot, send_sem, recv_sem, seat):
        return pltpu.make_async_remote_copy(
            src_ref=source,
            dst_ref=target_slot,
            send_sem=send_sem,
            recv_sem=recv_sem,
            device_id=(group, seat),
            device_id_type=MESH,
        )

    def z_copy(item):
        kind, hop, head = parts_of(item)
        return remote(
            slot(kind, head, hop),
            slot(kind, head, 2 * hop + 1),
            z_send.at[hop],
            z_recv.at[item],
            me + PLANE,
        )

    def y_copy(item):
        kind, half, head = parts_of(item)
        return remote(
            slot(kind, head, half + column * (half + 1)),
            slot(kind, head, 2 * half + 2),
            y_send.at[half],
            y_recv.at[item],
            beside,
        )

    def pair_copy(kind, position, batch, heads):
        start = pl.multiple_of(position * unit + core * rows, rows)
        place = held.at[kind, pl.ds(batch * heads, heads), pl.ds(start, rows), :]
        index = (kind, position, batch)
        return remote(place, place, pair_send.at[position], pair_recv.at[index], partner)

    def all_sent(sem):
        every = held.at[:, :, pl.ds(0, rows), :]
        remote(every, every, sem, sem, partner).wait_send()

    def own_arrived(kind):
        every = held.at[kind, :, pl.ds(pl.multiple_of(core * rows, rows), rows), :]
        pltpu.make_async_copy(every, every, own_sem.at[kind]).wait()

    def y_sends(half):
        return plane >= half + column

    def y_takes(half):
        return plane >= half + 1 - column

    def start_own(kind):
        @pl.when(has_upper)
        def _():
            for head in range(KEY_VALUE_HEADS):
                z_copy(kind * 2 * KEY_VALUE_HEADS + head).start()

        @pl.when(column == 0)
        def _():
            for head in range(KEY_VALUE_HEADS):
                y_copy(kind * 2 * KEY_VALUE_HEADS + head).start()

    pl.semaphore_wait(
        barrier, 1 + has_upper.astype(jnp.int32) + (plane >= column).astype(jnp.int32)
    )
    own_arrived(0)
    start_own(0)
    pair_copy(0, 0, 0, KEY_VALUE_HEADS).start()
    own_arrived(1)
    pair_copy(1, 0, 0, KEY_VALUE_HEADS).start()

    @pl.when(plane == 0)
    def _():
        start_own(1)

    length_copy.wait()
    place = lax.broadcasted_iota(jnp.int32, (rows, unit), 0) + me * rows
    bound = jnp.int32(0)
    begin = jnp.zeros((rows, unit), jnp.int32)
    for document in range(lengths_ref.shape[0] - 1):
        bound = bound + lengths_ref[document]
        begin = jnp.where(place >= bound, bound, begin)
    nothing = jnp.zeros((2, KEY_VALUE_HEADS, unit, HEAD_WIDTH), held.dtype)
    for position, distance in enumerate(DISTANCES):
        spot = pl.ds(position * unit, unit)
        key_place = lax.broadcasted_iota(jnp.int32, (rows, unit), 1) + (chip - distance) * unit
        visible = (key_place >= begin) & (key_place <= place)
        bias[:, spot] = jnp.where(visible, 0.0, HIDDEN)

        @pl.when(chip < distance)
        def _():
            held[:, :, spot, :] = nothing

    def weigh(head, team, room):
        spot = pl.ds(TEAMS[team][0] * unit, TEAMS[team][1] * unit)
        width = TEAMS[team][1] * unit
        keys = held[0, head, spot, :]
        half = stacked // 2
        for first in range(0, stacked, half):
            scores[room, pl.ds(first, half), 0:width] = lax.dot_general(
                queries[head, pl.ds(first, half), :],
                keys,
                (((1,), (1,)), ((), ())),
                preferred_element_type=jnp.float32,
            )
        step = rows // 4
        for first in range(0, stacked, step):
            span = pl.ds(first, step)
            masked = scores[room, span, 0:width] + bias[pl.ds(first % rows, step), spot]
            top = jnp.max(masked, axis=1, keepdims=True)
            weights[head, span, spot] = jnp.exp2((masked - top) * factor).astype(jnp.bfloat16)
            spread = jnp.broadcast_to(top, (step, HEAD_WIDTH))
            tops[head, team, span, :] = spread
            if team == 0:
                highest[head, span, :] = spread
            else:
                highest[head, span, :] = jnp.maximum(highest[head, span, :], spread)

    def blend(head, team):
        spot = pl.ds(TEAMS[team][0] * unit, TEAMS[team][1] * unit)
        values = held[1, head, spot, :]
        product = jnp.dot(
            weights[head, :, spot],
            jnp.concatenate([values, jnp.ones_like(values)], axis=1),
            preferred_element_type=jnp.float32,
        )
        step = rows // 2
        for first in range(0, stacked, step):
            span = pl.ds(first, step)
            share = jnp.exp2((tops[head, team, span, :] - highest[head, span, :]) * factor)
            part = product[first : first + step] * jnp.concatenate([share, share], axis=1)
            if team == 0:
                total[head, span, :] = part
            else:
                total[head, span, :] = total[head, span, :] + part

    outputs = (first_out, second_out)

    def finish(head):
        for layer in range(2):
            for member in range(SHARE):
                span = pl.ds((layer * SHARE + member) * rows, rows)
                blended = total[head, span, 0:HEAD_WIDTH] / total[head, span, HEAD_WIDTH:]
                start = pl.multiple_of((head * SHARE + member) * HEAD_WIDTH, HEAD_WIDTH)
                outputs[layer][:, pl.ds(start, HEAD_WIDTH)] = blended.astype(jnp.bfloat16)

    pltpu.make_async_copy(queries, queries, query_sem).wait()

    batches = KEY_VALUE_HEADS // BATCH
    pair_items = 4 * batches

    def batch_parts(item):
        return item // (2 * batches), (item // batches) % 2, item % batches

    def z_ready(item):
        kind, hop, batch = batch_parts(item)

        @pl.when((item >= 0) & (item < pair_items) & (plane >= hop + 1))
        def _():
            pair_copy(kind, 2 * hop + 1, batch, BATCH).wait_recv()

    def y_ready(item):
        kind, half, batch = batch_parts(item)

        @pl.when((item >= 0) & (item < pair_items) & y_takes(half))
        def _():
            pair_copy(kind, 2 * half + 2, batch, BATCH).wait_recv()

    def z_arrival(item):
        kind, hop, batch = batch_parts(item)

        @pl.when((item < pair_items) & (plane >= hop + 1))
        def _():
            for piece in range(BATCH):
                chunk = item * BATCH + piece
                z_copy(chunk).wait_recv()

                @pl.when((column == 1) | (hop == 0))
                def _():
                    y_copy(chunk + KEY_VALUE_HEADS * (1 - column)).start()

                @pl.when(has_upper & (hop == 0))
                def _():
                    z_copy(chunk + KEY_VALUE_HEADS).start()

            pair_copy(kind, 2 * hop + 1, batch, BATCH).start()

        @pl.when((item == batches - 1) & (plane >= 1))
        def _():
            start_own(1)

    def y_arrival(item):
        kind, half, batch = batch_parts(item)

        @pl.when((item >= 0) & (item < pair_items) & y_takes(half))
        def _():
            for piece in range(BATCH):
                y_copy(item * BATCH + piece).wait_recv()
            pair_copy(kind, 2 * half + 2, batch, BATCH).start()

    def step(index, carry):
        z_arrival(index)
        y_arrival(index - Y_LAG)
        z_ready(index - Z_PAIR_LAG)
        y_ready(index - Y_PAIR_LAG)
        for kind, stages in ((0, WEIGH_STEPS), (1, BLEND_STEPS)):
            for team, begin in enumerate(stages):

                @pl.when((index >= begin) & (index < begin + batches))
                def _():
                    if team == 0:

                        @pl.when(index == begin)
                        def _():
                            pair_copy(kind, 0, 0, KEY_VALUE_HEADS).wait_recv()

                    for piece in range(BATCH):
                        head = (index - begin) * BATCH + piece
                        if kind == 0:
                            weigh(head, team, piece)
                        else:
                            blend(head, team)
                    if kind == 1 and team == len(TEAMS) - 1:
                        for piece in range(BATCH):
                            finish((index - begin) * BATCH + piece)

        return carry

    lax.fori_loop(0, BLEND_STEPS[-1] + batches, step, 0)

    for hop in range(2):

        @pl.when(has_upper & (plane >= hop))
        def _():
            all_sent(z_send.at[hop])

        @pl.when(y_sends(hop))
        def _():
            all_sent(y_send.at[hop])

    for position, distance in enumerate(DISTANCES):

        @pl.when(chip >= distance)
        def _():
            all_sent(pair_send.at[position])


def on_device(first_queries, second_queries, common_keys, common_values, lengths):
    planes = lax.axis_size("seq") // PLANE
    rows = common_keys.shape[0]
    unit = CORES * rows
    units = REACH + 1
    stacked = 2 * SHARE * rows
    in_vmem = pl.BlockSpec(memory_space=pltpu.VMEM)
    anywhere = pl.BlockSpec(memory_space=pl.ANY)
    shape = pltpu.VMEM(first_queries.shape, jnp.bfloat16)
    placed = pl.pallas_call(
        functools.partial(kernel, planes),
        out_shape=(shape, shape),
        in_specs=[anywhere] * 5,
        out_specs=(in_vmem, in_vmem),
        scratch_shapes=[
            pltpu.VMEM((KEY_VALUE_HEADS, stacked, HEAD_WIDTH), jnp.bfloat16),
            pltpu.VMEM((2, KEY_VALUE_HEADS, units * unit, HEAD_WIDTH), jnp.bfloat16),
            pltpu.VMEM((rows, units * unit), jnp.float32),
            pltpu.VMEM((BATCH, stacked, 2 * unit), jnp.float32),
            pltpu.VMEM((KEY_VALUE_HEADS, stacked, units * unit), jnp.bfloat16),
            pltpu.VMEM((KEY_VALUE_HEADS, len(TEAMS), stacked, HEAD_WIDTH), jnp.float32),
            pltpu.VMEM((KEY_VALUE_HEADS, stacked, HEAD_WIDTH), jnp.float32),
            pltpu.VMEM((KEY_VALUE_HEADS, stacked, 2 * HEAD_WIDTH), jnp.float32),
            pltpu.SMEM(lengths.shape, lengths.dtype),
            pltpu.SemaphoreType.DMA,
            pltpu.SemaphoreType.DMA((2,)),
            pltpu.SemaphoreType.DMA,
            pltpu.SemaphoreType.DMA((2,)),
            pltpu.SemaphoreType.DMA((4 * KEY_VALUE_HEADS,)),
            pltpu.SemaphoreType.DMA((2,)),
            pltpu.SemaphoreType.DMA((4 * KEY_VALUE_HEADS,)),
            pltpu.SemaphoreType.DMA((units,)),
            pltpu.SemaphoreType.DMA((2, units, KEY_VALUE_HEADS // BATCH)),
        ],
        compiler_params=pltpu.CompilerParams(collective_id=0, has_side_effects=True),
    )(lengths, first_queries, second_queries, common_keys, common_values)
    return to_memory(*placed)


def place_outputs(first_ref, second_ref, first_out, second_out, sems):
    copies = [
        pltpu.make_async_copy(source, target, sems.at[index])
        for index, (source, target) in enumerate(
            ((first_ref, first_out), (second_ref, second_out))
        )
    ]
    for copy in copies:
        copy.start()
    for copy in copies:
        copy.wait()


def to_memory(first, second):
    in_vmem = pl.BlockSpec(memory_space=pltpu.VMEM)
    anywhere = pl.BlockSpec(memory_space=pltpu.HBM)
    shape = jax.ShapeDtypeStruct(first.shape, first.dtype)
    return pl.pallas_call(
        place_outputs,
        out_shape=(shape, shape),
        in_specs=[in_vmem] * 2,
        out_specs=(anywhere, anywhere),
        scratch_shapes=[pltpu.SemaphoreType.DMA((2,))],
    )(
        pltpu.with_memory_space_constraint(first, pltpu.VMEM),
        pltpu.with_memory_space_constraint(second, pltpu.VMEM),
    )


def solution(mesh):
    in_specs = (
        P(("groups", "seq"), None),
        P(("groups", "seq"), None),
        P(("groups", "seq"), None),
        P(("groups", "seq"), None),
        P("groups"),
    )
    out_specs = (P(("groups", "seq"), None), P(("groups", "seq"), None))
    body = on_device if mesh.shape["seq"] == 2 * REACH * CORES else on_device_wide
    return jax.shard_map(
        body, mesh=mesh, in_specs=in_specs, out_specs=out_specs, check_vma=False
    )
```
